32 devices in a mesh: row: 16 (over z, x, core), col: 2 (over y).
Axes of the slice: x: 2, y: 2, z: 4, core: 2. Of those that a mesh axis runs over, the one named last changes fastest.
Arguments:
- species: float32 [2, 128, 128, 64], P(None, None, 'row', 'col'), may hold values from -6 to 6
- symbol_x: float32 [128], replicated, may hold values from 0.3 to 3
- symbol_y: float32 [128], replicated, may hold values from 0.3 to 3
- symbol_z: float32 [64], replicated, may hold values from 0.3 to 3
Outputs:
- spectrum: float32 [2, 128, 128, 64], P(None, 'row', 'col')
The draws below stay inside these ranges and needn't reach their ends.
All inputs are finite; a program needn't handle non-finite values.
Results may differ from the reference program's by a relative error of at most 0.00007.
Values sent between devices are 32-bit elements; how exact they have to be, the bound alone decides.
No kernel may reach another device: no remote copies, remote signals or barrier semaphores. Data moves between devices by JAX's collectives and lax.ppermute only.
A program may use at most 64 MiB of HBM per device.

```python
import jax
import jax.numpy as jnp
from jax import lax

GRID_X = 128
GRID_Y = 128
GRID_Z = 64
FIELDS = 2


def level_of(own_key, extent, split, least, high):
    def one(position, shards_of):
        heights = jax.random.uniform(jax.random.fold_in(jax.random.fold_in(own_key, 6), position), (shards_of,), jnp.float32, least / len(split), high / len(split))
        return jnp.repeat(jnp.exp(heights), extent[position] // shards_of).reshape((-1,) + (1,) * (len(extent) - position - 1))

    level = one(*split[0])
    for cut in split[1:]:
        level = level * one(*cut)
    return level


def centred(rng, shape, scale, most, cuts=(), held_as=jnp.bfloat16):
    entries = jax.random.normal(rng, shape, jnp.float32) * scale
    if len(cuts) > 0:
        entries = level_of(rng, shape, cuts, -0.22, 0.18) * entries
    return jnp.clip(entries, min=-most, max=most).astype(held_as)


def setup_inputs(seed: int = 0) -> dict:
    key_of = jax.random.split(jax.random.key(seed), 5)
    return {
        "species": centred(key_of[0], (FIELDS, GRID_X, GRID_Y, GRID_Z), 1.0, 6.0, ((2, 16), (3, 2)), jnp.float32),
        "symbol_x": jnp.clip(jax.random.uniform(key_of[1], (GRID_X,), jnp.float32, 0.3, 3.0), 0.3, 3.0),
        "symbol_y": jnp.clip(jax.random.uniform(key_of[2], (GRID_Y,), jnp.float32, 0.3, 3.0), 0.3, 3.0),
        "symbol_z": jnp.clip(jax.random.uniform(key_of[3], (GRID_Z,), jnp.float32, 0.3, 3.0), 0.3, 3.0),
    }


def basis_table(count):
    rank = jnp.arange(count)
    angle = (jnp.pi / (4 * count)) * (((2 * rank[:, None] + 1) * (2 * rank[None, :] + 1)) % (8 * count)).astype(jnp.float32)
    return jnp.cos(angle) * (2.0 / count) ** 0.5


def to_modes(values, dim):
    moved = jnp.tensordot(values, basis_table(values.shape[dim]), axes=([dim], [0]), precision=lax.Precision.HIGHEST)
    return jnp.moveaxis(moved, -1, dim)


def reference(species, symbol_x, symbol_y, symbol_z):
    spectrum = species
    spectrum = to_modes(spectrum, 1)
    spectrum = to_modes(spectrum, 2)
    spectrum = to_modes(spectrum, 3)
    symbol = symbol_x[:, None, None] + symbol_y[None, :, None] + symbol_z[None, None, :]
    spectrum = spectrum / symbol
    return spectrum
```

```python
import functools

import jax
import jax.numpy as jnp
import numpy as np
from jax import lax
from jax.experimental import pallas as pl
from jax.experimental.pallas import tpu as pltpu
from jax.sharding import PartitionSpec as P

LANES = 128
SUBLANES = 8
VMEM_GRANT = 12 * 2**20
VMEM = pl.BlockSpec(memory_space=pltpu.VMEM)
SMEM = pl.BlockSpec(memory_space=pltpu.SMEM)


def basis_table(count):
    rank = np.arange(count)
    odd = 2 * rank + 1
    angle = np.pi / (4 * count) * (odd[:, None] * odd[None, :] % (8 * count))
    return (np.cos(angle) * (2.0 / count) ** 0.5).astype(np.float32)


def split_table(table):
    high = table.astype(jnp.bfloat16)
    low = (table - high.astype(np.float32)).astype(jnp.bfloat16)
    return high, low


def split(values):
    high = values.astype(jnp.bfloat16)
    low = (values - high.astype(jnp.float32)).astype(jnp.bfloat16)
    return high, low


def dot(left, right):
    return jnp.dot(left, right, preferred_element_type=jnp.float32)


def dot_nt(left, right):
    return lax.dot_general(
        left, right, (((1,), (1,)), ((), ())), preferred_element_type=jnp.float32
    )


def x_kernel(a_ref, h_ref, o_ref):
    fields, ys, zs, _ = a_ref.shape
    half = fields * zs
    parts = LANES // half
    rows = h_ref.shape[0] // parts
    table = h_ref[...]
    lane = lax.broadcasted_iota(jnp.int32, (rows, LANES), 1)
    for y in range(ys):
        a = jnp.concatenate([a_ref[f, y] for f in range(fields)] * parts, axis=0)
        high, low = split(a)
        c = dot_nt(table, jnp.concatenate([high, high, low], axis=1))
        out = c[:rows]
        for part in range(1, parts):
            out = jnp.where(lane < part * half, out, c[part * rows : (part + 1) * rows])
        o_ref[pl.ds(y, rows, stride=ys), :] = out


def y_products(r_ref, table):
    count, k_lo, ys, lanes = r_ref.shape
    outs = []
    for k in range(k_lo):
        r = r_ref[:, k].reshape(count * ys, lanes)
        high, low = split(r)
        outs.append(dot(table, jnp.concatenate([high, high, low], axis=0)))
    return outs


def y_send_kernel(cols, r_ref, h_ref, *o_refs):
    me = lax.axis_index("col")
    for step, o_ref in enumerate(o_refs, 1):
        target = lax.rem(me + step, cols)
        for k, out in enumerate(y_products(r_ref, h_ref[target])):
            o_ref[k] = out


def y_keep_kernel(cols, r_ref, h_ref, w_ref, sx_ref, sy_ref, sz_ref, o_ref, inv_ref, sy_scr):
    me = lax.axis_index("col")
    row = lax.axis_index("row")
    fields, share_x, share_y, nz = o_ref.shape
    k_lo = r_ref.shape[1]
    parts = share_x // k_lo
    ny = sy_ref.shape[1]
    for i in range(ny // LANES):
        sy_scr[i * LANES : (i + 1) * LANES, :] = jnp.broadcast_to(
            sy_ref[:, i * LANES : (i + 1) * LANES], (LANES, LANES)
        ).T
    sy = sy_scr[pl.ds(me * share_y, share_y), :][:, :1]
    sz = sz_ref[...]
    plane = sy + sz
    for k in range(share_x):
        inv_ref[k] = 1.0 / (sx_ref[row * share_x + k] + plane)
    weights = w_ref[me]
    for k, out in enumerate(y_products(r_ref, h_ref[me])):
        high, low = split(out)
        c = dot(jnp.concatenate([high, high, low], axis=1), weights)
        pad = c.shape[1] // (parts * fields)
        for part in range(parts):
            for f in range(fields):
                at = (part * fields + f) * pad
                o_ref[f, part * k_lo + k] = c[:, at : at + nz]


def z_kernel(cols, *refs):
    p_refs = refs[: cols - 1]
    acc_ref, inv_ref, w_ref, o_ref = refs[cols - 1 :]
    me = lax.axis_index("col")
    fields, share_x, share_y, nz = o_ref.shape
    k_lo = p_refs[0].shape[0]
    parts = share_x // k_lo
    for k in range(k_lo):
        c = None
        for step, p_ref in enumerate(p_refs, 1):
            source = lax.rem(me + cols - step, cols)
            high, low = split(p_ref[k])
            term = dot(jnp.concatenate([high, high, low], axis=1), w_ref[source])
            c = term if c is None else c + term
        pad = c.shape[1] // (parts * fields)
        for part in range(parts):
            for f in range(fields):
                at = (part * fields + f) * pad
                kx = part * k_lo + k
                o_ref[f, kx] = (acc_ref[f, kx] + c[:, at : at + nz]) * inv_ref[kx]


def call(kernel, out_shape, ins, outs, scratch=(), flops=0, bytes_accessed=0):
    return pl.pallas_call(
        kernel,
        out_shape=out_shape,
        in_specs=ins,
        out_specs=outs,
        scratch_shapes=scratch,
        compiler_params=pltpu.CompilerParams(vmem_limit_bytes=VMEM_GRANT),
        cost_estimate=pl.CostEstimate(
            flops=flops, bytes_accessed=bytes_accessed, transcendentals=0
        ),
    )


def f32(*shape):
    return jax.ShapeDtypeStruct(shape, jnp.float32)


def on_device(rows, cols, species, symbol_x, symbol_y, symbol_z):
    fields, nx, share_in, zs = species.shape
    ny, nz = share_in * rows, zs * cols
    share_x, share_y = nx // rows, ny // cols
    parts = LANES // (fields * zs)
    k_lo = share_x // parts
    assert parts * fields * zs == LANES and k_lo * parts == share_x
    assert share_in == SUBLANES

    hx = basis_table(nx).reshape(rows, parts, k_lo, nx).transpose(1, 0, 2, 3).reshape(nx, nx)
    high, low = split_table(hx)
    hx3 = jnp.asarray(np.concatenate([high, low, high], axis=1))
    high, low = split_table(basis_table(ny))
    hy3 = jnp.asarray(np.concatenate([high, low, high], axis=1).reshape(cols, share_y, 3 * ny))
    hz = basis_table(nz).reshape(cols, zs, nz)
    pad = -(-nz // LANES) * LANES
    wz = np.zeros((cols, parts * fields, zs, parts * fields, pad), np.float32)
    for j in range(parts * fields):
        wz[:, j, :, j, :nz] = hz
    wz = wz.reshape(cols, LANES, parts * fields * pad)
    high, low = split_table(wz)
    wz3 = jnp.asarray(np.concatenate([high, low, high], axis=1))

    send = call(
        x_kernel,
        f32(nx // parts * share_in, LANES),
        [VMEM, VMEM],
        VMEM,
        flops=6 * nx * nx * fields * share_in * zs,
        bytes_accessed=8 * species.size,
    )(jnp.transpose(species, (0, 2, 3, 1)), hx3)
    got = lax.all_to_all(
        send.reshape(rows, k_lo * share_in, LANES), "row", split_axis=0, concat_axis=0, tiled=True
    ).reshape(rows, k_lo, share_in, LANES)

    pieces = call(
        functools.partial(y_send_kernel, cols),
        [f32(k_lo, share_y, LANES)] * (cols - 1),
        [VMEM, VMEM],
        [VMEM] * (cols - 1),
        flops=6 * share_y * ny * k_lo * LANES * (cols - 1),
        bytes_accessed=8 * species.size,
    )(got, hy3)
    arrived = [
        lax.ppermute(piece, "col", [(d, (d + step) % cols) for d in range(cols)])
        for step, piece in enumerate(pieces, 1)
    ]
    kept, inverse = call(
        functools.partial(y_keep_kernel, cols),
        [f32(fields, share_x, share_y, nz), f32(share_x, share_y, nz)],
        [VMEM, VMEM, VMEM, SMEM, VMEM, VMEM],
        [VMEM, VMEM],
        scratch=[pltpu.VMEM((ny, LANES), jnp.float32)],
        flops=6 * share_y * ny * k_lo * LANES * 4,
        bytes_accessed=16 * species.size,
    )(got, hy3, wz3, symbol_x, symbol_y.reshape(1, ny), symbol_z.reshape(1, nz))
    return call(
        functools.partial(z_kernel, cols),
        f32(fields, share_x, share_y, nz),
        [VMEM] * (cols + 2),
        VMEM,
        flops=6 * share_y * share_x * fields * nz * nz,
        bytes_accessed=16 * species.size,
    )(*arrived, kept, inverse, wz3)


def solution(mesh):
    rows, cols = mesh.shape["row"], mesh.shape["col"]
    in_specs = (P(None, None, "row", "col"), P(), P(), P())
    out_specs = P(None, "row", "col", None)
    return jax.shard_map(
        functools.partial(on_device, rows, cols),
        mesh=mesh,
        in_specs=in_specs,
        out_specs=out_specs,
        check_vma=False,
    )
```

```python
import functools

import jax
import jax.numpy as jnp
import numpy as np
from jax import lax
from jax.experimental import pallas as pl
from jax.experimental.pallas import tpu as pltpu
from jax.sharding import PartitionSpec as P

LANES = 128
SUBLANES = 8
VMEM_GRANT = 12 * 2**20
Y_STEP = 2
GROUPS = 2
VMEM = pl.BlockSpec(memory_space=pltpu.VMEM)
SMEM = pl.BlockSpec(memory_space=pltpu.SMEM)
HBM = pl.BlockSpec(memory_space=pltpu.HBM)


def basis_table(count):
    rank = np.arange(count)
    odd = 2 * rank + 1
    angle = np.pi / (4 * count) * (odd[:, None] * odd[None, :] % (8 * count))
    return (np.cos(angle) * (2.0 / count) ** 0.5).astype(np.float32)


def split_table(table):
    high = table.astype(jnp.bfloat16)
    low = (table - high.astype(np.float32)).astype(jnp.bfloat16)
    return high, low


def split(values):
    high = values.astype(jnp.bfloat16)
    low = (values - high.astype(jnp.float32)).astype(jnp.bfloat16)
    return high, low


def dot(left, right):
    return jnp.dot(left, right, preferred_element_type=jnp.float32)


def dot_nt(left, right):
    return lax.dot_general(
        left, right, (((1,), (1,)), ((), ())), preferred_element_type=jnp.float32
    )


def x_kernel(a_hbm, h_hbm, o_ref, a_ref, h_ref, a_sems, h_sem):
    fields, ys, zs, nx = a_ref.shape
    half = fields * zs
    parts = LANES // half
    rows = h_ref.shape[0] // parts
    table_copy = pltpu.make_async_copy(h_hbm, h_ref, h_sem)
    table_copy.start()
    copies = []
    for i in range(0, ys, Y_STEP):
        at = (slice(None), pl.ds(i, Y_STEP))
        copies.append(pltpu.make_async_copy(a_hbm.at[at], a_ref.at[at], a_sems.at[i // Y_STEP]))
        copies[-1].start()
    table_copy.wait()
    table = jnp.concatenate([h_ref[...], h_ref[:, :nx]], axis=1)
    lane = lax.broadcasted_iota(jnp.int32, (rows, LANES), 1)
    for i in range(0, ys, Y_STEP):
        copies[i // Y_STEP].wait()
        a = [a_ref[f, y] for y in range(i, i + Y_STEP) for _ in range(parts) for f in range(fields)]
        high, low = split(jnp.concatenate(a, axis=0))
        c = dot_nt(table, jnp.concatenate([high, high, low], axis=1))
        for j in range(Y_STEP):
            mine = c[:, j * LANES : (j + 1) * LANES]
            out = mine[:rows]
            for part in range(1, parts):
                out = jnp.where(lane < part * half, out, mine[part * rows : (part + 1) * rows])
            o_ref[pl.ds(i + j, rows, stride=ys), :] = out


def y_products(r_ref, h_ref, target, ks):
    count, _, ys, lanes = r_ref.shape
    table = h_ref[target]
    table = jnp.concatenate([table, table[:, : count * ys]], axis=1)
    outs = []
    for k in ks:
        high, low = split(r_ref[:, k].reshape(count * ys, lanes))
        outs.append(dot(table, jnp.concatenate([high, high, low], axis=0)))
    return outs


def y_send_kernel(cols, ks, r_ref, h_ref, *o_refs):
    me = lax.axis_index("col")
    for step, o_ref in enumerate(o_refs, 1):
        target = lax.rem(me + step, cols)
        for i, out in enumerate(y_products(r_ref, h_ref, target, ks)):
            o_ref[i] = out


def z_products(p, weights):
    high, low = split(p)
    return dot(jnp.concatenate([high, high, low], axis=1), weights)


def y_keep_kernel(cols, r_ref, h_ref, w_ref, sx_ref, sy_ref, sz_ref, o_ref, inv_ref, sy_scr):
    me = lax.axis_index("col")
    row = lax.axis_index("row")
    fields, share_x, share_y, nz = o_ref.shape
    k_lo = r_ref.shape[1]
    parts = share_x // k_lo
    ny = sy_ref.shape[1]
    for i in range(ny // LANES):
        sy_scr[i * LANES : (i + 1) * LANES, :] = jnp.broadcast_to(
            sy_ref[:, i * LANES : (i + 1) * LANES], (LANES, LANES)
        ).T
    sy = sy_scr[pl.ds(me * share_y, share_y), :][:, :1]
    plane = sy + sz_ref[...]
    for k in range(share_x):
        inv_ref[k] = 1.0 / (sx_ref[row * share_x + k] + plane)
    weights = w_ref[me]
    for k, out in enumerate(y_products(r_ref, h_ref, me, range(k_lo))):
        c = z_products(out, weights)
        pad = c.shape[1] // (parts * fields)
        for part in range(parts):
            for f in range(fields):
                at = (part * fields + f) * pad
                o_ref[f, part * k_lo + k] = c[:, at : at + nz]


def z_kernel(cols, k_lo, ks, *refs):
    p_refs = refs[: cols - 1]
    acc_ref, inv_ref, w_ref = refs[cols - 1 : cols + 2]
    o_hbm, o_ref, sems = refs[-3:]
    me = lax.axis_index("col")
    fields, share_x, share_y, nz = acc_ref.shape
    parts = share_x // k_lo
    copies = []
    for i, k in enumerate(ks):
        c = None
        for step, p_ref in enumerate(p_refs, 1):
            source = lax.rem(me + cols - step, cols)
            term = z_products(p_ref[i], w_ref[source])
            c = term if c is None else c + term
        pad = c.shape[1] // (parts * fields)
        for part in range(parts):
            for f in range(fields):
                at = (part * fields + f) * pad
                kx = part * k_lo + k
                slot = (i * parts + part) * fields + f
                o_ref[slot] = (acc_ref[f, kx] + c[:, at : at + nz]) * inv_ref[kx]
                copies.append(
                    pltpu.make_async_copy(o_ref.at[slot], o_hbm.at[f, kx], sems.at[slot])
                )
                copies[-1].start()
    for copy in copies:
        copy.wait()


def call(kernel, out_shape, ins, outs, scratch=(), flops=0, bytes_accessed=0, aliases=None):
    return pl.pallas_call(
        kernel,
        out_shape=out_shape,
        in_specs=ins,
        out_specs=outs,
        scratch_shapes=scratch,
        input_output_aliases=aliases or {},
        compiler_params=pltpu.CompilerParams(vmem_limit_bytes=VMEM_GRANT),
        cost_estimate=pl.CostEstimate(
            flops=flops, bytes_accessed=bytes_accessed, transcendentals=0
        ),
    )


def f32(*shape):
    return jax.ShapeDtypeStruct(shape, jnp.float32)


def on_device(rows, cols, species, symbol_x, symbol_y, symbol_z):
    fields, nx, share_in, zs = species.shape
    ny, nz = share_in * rows, zs * cols
    share_x, share_y = nx // rows, ny // cols
    parts = LANES // (fields * zs)
    k_lo = share_x // parts
    assert parts * fields * zs == LANES and k_lo * parts == share_x
    assert share_in == SUBLANES

    hx = basis_table(nx).reshape(rows, parts, k_lo, nx).transpose(1, 0, 2, 3).reshape(nx, nx)
    high, low = split_table(hx)
    hx2 = jnp.asarray(np.concatenate([high, low], axis=1))
    high, low = split_table(basis_table(ny))
    hy2 = jnp.asarray(np.concatenate([high, low], axis=1).reshape(cols, share_y, 2 * ny))
    hz = basis_table(nz).reshape(cols, zs, nz)
    pad = -(-nz // LANES) * LANES
    wz = np.zeros((cols, parts * fields, zs, parts * fields, pad), np.float32)
    for j in range(parts * fields):
        wz[:, j, :, j, :nz] = hz
    wz = wz.reshape(cols, LANES, parts * fields * pad)
    high, low = split_table(wz)
    wz3 = jnp.asarray(np.concatenate([high, low, high], axis=1))

    moved = jnp.transpose(species, (0, 2, 3, 1))
    send = call(
        x_kernel,
        f32(nx // parts * share_in, LANES),
        [HBM, HBM],
        VMEM,
        scratch=[
            pltpu.VMEM(moved.shape, jnp.float32),
            pltpu.VMEM(hx2.shape, jnp.bfloat16),
            pltpu.SemaphoreType.DMA((share_in // Y_STEP,)),
            pltpu.SemaphoreType.DMA,
        ],
        flops=6 * nx * nx * fields * share_in * zs,
        bytes_accessed=8 * species.size,
    )(pltpu.with_memory_space_constraint(moved, pltpu.HBM), pltpu.with_memory_space_constraint(hx2, pltpu.HBM))
    got = lax.all_to_all(
        send.reshape(rows, k_lo * share_in, LANES), "row", split_axis=0, concat_axis=0, tiled=True
    ).reshape(rows, k_lo, share_in, LANES)

    size = k_lo // GROUPS
    groups = [range(g * size, (g + 1) * size) for g in range(GROUPS)]
    arrived = []
    for ks in groups:
        pieces = call(
            functools.partial(y_send_kernel, cols, ks),
            [f32(size, share_y, LANES)] * (cols - 1),
            [VMEM, VMEM],
            [VMEM] * (cols - 1),
            flops=6 * share_y * ny * size * LANES * (cols - 1),
            bytes_accessed=8 * species.size // GROUPS,
        )(got, hy2)
        arrived.append(
            [
                lax.ppermute(piece, "col", [(d, (d + step) % cols) for d in range(cols)])
                for step, piece in enumerate(pieces, 1)
            ]
        )
    kept, inverse = call(
        functools.partial(y_keep_kernel, cols),
        [f32(fields, share_x, share_y, nz), f32(share_x, share_y, nz)],
        [VMEM, VMEM, VMEM, SMEM, VMEM, VMEM],
        [VMEM, VMEM],
        scratch=[pltpu.VMEM((ny, LANES), jnp.float32)],
        flops=6 * share_y * ny * k_lo * LANES * 4,
        bytes_accessed=16 * species.size,
    )(got, hy2, wz3, symbol_x, symbol_y.reshape(1, ny), symbol_z.reshape(1, nz))
    out = None
    slots = size * parts * fields
    for ks, parts_in in zip(groups, arrived):
        args = [*parts_in, kept, inverse, wz3] + ([] if out is None else [out])
        out = call(
            functools.partial(z_kernel, cols, k_lo, ks),
            f32(fields, share_x, share_y, nz),
            [VMEM] * (cols + 2) + ([] if out is None else [HBM]),
            HBM,
            scratch=[
                pltpu.VMEM((slots, share_y, nz), jnp.float32),
                pltpu.SemaphoreType.DMA((slots,)),
            ],
            flops=6 * share_y * share_x * fields * nz * nz // GROUPS,
            bytes_accessed=16 * species.size // GROUPS,
            aliases={} if out is None else {cols + 2: 0},
        )(*args)
    return out


def solution(mesh):
    rows, cols = mesh.shape["row"], mesh.shape["col"]
    in_specs = (P(None, None, "row", "col"), P(), P(), P())
    out_specs = P(None, "row", "col", None)
    return jax.shard_map(
        functools.partial(on_device, rows, cols),
        mesh=mesh,
        in_specs=in_specs,
        out_specs=out_specs,
        check_vma=False,
    )
```

```python
import functools

import jax
import jax.numpy as jnp
import numpy as np
from jax import lax
from jax.experimental import pallas as pl
from jax.experimental.pallas import tpu as pltpu
from jax.sharding import PartitionSpec as P

LANES = 128
SUBLANES = 8
VMEM_GRANT = 12 * 2**20
Y_STEP = 2
GROUPS = 1
VMEM = pl.BlockSpec(memory_space=pltpu.VMEM)
SMEM = pl.BlockSpec(memory_space=pltpu.SMEM)
HBM = pl.BlockSpec(memory_space=pltpu.HBM)


def basis_table(count):
    rank = np.arange(count)
    odd = 2 * rank + 1
    angle = np.pi / (4 * count) * (odd[:, None] * odd[None, :] % (8 * count))
    return (np.cos(angle) * (2.0 / count) ** 0.5).astype(np.float32)


def split_table(table):
    high = table.astype(jnp.bfloat16)
    low = (table - high.astype(np.float32)).astype(jnp.bfloat16)
    return high, low


def split(values):
    high = values.astype(jnp.bfloat16)
    low = (values - high.astype(jnp.float32)).astype(jnp.bfloat16)
    return high, low


def dot(left, right):
    return jnp.dot(left, right, preferred_element_type=jnp.float32)


def dot_nt(left, right):
    return lax.dot_general(
        left, right, (((1,), (1,)), ((), ())), preferred_element_type=jnp.float32
    )


def x_kernel(a_hbm, h_hbm, o_ref, a_ref, h_ref, a_sem, h_sem):
    fields, ys, zs, nx = a_ref.shape
    half = fields * zs
    parts = LANES // half
    rows = h_ref.shape[0] // parts
    copies = [
        pltpu.make_async_copy(h_hbm, h_ref, h_sem),
        pltpu.make_async_copy(a_hbm, a_ref, a_sem),
    ]
    for copy in copies:
        copy.start()
    for copy in copies:
        copy.wait()
    table = jnp.concatenate([h_ref[...], h_ref[:, :nx]], axis=1)
    lane = lax.broadcasted_iota(jnp.int32, (rows, LANES), 1)
    for i in range(0, ys, Y_STEP):
        a = [a_ref[f, y] for y in range(i, i + Y_STEP) for _ in range(parts) for f in range(fields)]
        high, low = split(jnp.concatenate(a, axis=0))
        c = dot_nt(table, jnp.concatenate([high, high, low], axis=1))
        for j in range(Y_STEP):
            mine = c[:, j * LANES : (j + 1) * LANES]
            out = mine[:rows]
            for part in range(1, parts):
                out = jnp.where(lane < part * half, out, mine[part * rows : (part + 1) * rows])
            o_ref[pl.ds(i + j, rows, stride=ys), :] = out


def y_products(r_ref, h_ref, target, ks):
    count, _, ys, lanes = r_ref.shape
    table = h_ref[target]
    table = jnp.concatenate([table, table[:, : count * ys]], axis=1)
    outs = []
    for k in ks:
        high, low = split(r_ref[:, k].reshape(count * ys, lanes))
        outs.append(dot(table, jnp.concatenate([high, high, low], axis=0)))
    return outs


def y_send_kernel(cols, ks, r_ref, h_ref, *o_refs):
    me = lax.axis_index("col")
    for step, o_ref in enumerate(o_refs, 1):
        target = lax.rem(me + step, cols)
        for i, out in enumerate(y_products(r_ref, h_ref, target, ks)):
            o_ref[i] = out


def z_products(p, weights):
    high, low = split(p)
    return dot(jnp.concatenate([high, high, low], axis=1), weights)


def y_keep_kernel(cols, r_ref, h_ref, w_ref, sx_ref, sy_ref, sz_ref, o_ref, inv_ref, sy_scr):
    me = lax.axis_index("col")
    row = lax.axis_index("row")
    fields, share_x, share_y, nz = o_ref.shape
    k_lo = r_ref.shape[1]
    parts = share_x // k_lo
    ny = sy_ref.shape[1]
    for i in range(ny // LANES):
        sy_scr[i * LANES : (i + 1) * LANES, :] = jnp.broadcast_to(
            sy_ref[:, i * LANES : (i + 1) * LANES], (LANES, LANES)
        ).T
    sy = sy_scr[pl.ds(me * share_y, share_y), :][:, :1]
    plane = sy + sz_ref[...]
    for k in range(share_x):
        inv_ref[k] = 1.0 / (sx_ref[row * share_x + k] + plane)
    weights = w_ref[me]
    for k, out in enumerate(y_products(r_ref, h_ref, me, range(k_lo))):
        c = z_products(out, weights)
        pad = c.shape[1] // (parts * fields)
        for part in range(parts):
            for f in range(fields):
                at = (part * fields + f) * pad
                o_ref[f, part * k_lo + k] = c[:, at : at + nz]


def z_kernel(cols, k_lo, ks, *refs):
    p_refs = refs[: cols - 1]
    acc_ref, inv_ref, w_ref = refs[cols - 1 : cols + 2]
    o_hbm, o_ref, sems = refs[-3:]
    me = lax.axis_index("col")
    fields, share_x, share_y, nz = acc_ref.shape
    parts = share_x // k_lo
    copies = []
    for i, k in enumerate(ks):
        c = None
        for step, p_ref in enumerate(p_refs, 1):
            source = lax.rem(me + cols - step, cols)
            term = z_products(p_ref[i], w_ref[source])
            c = term if c is None else c + term
        pad = c.shape[1] // (parts * fields)
        for part in range(parts):
            for f in range(fields):
                at = (part * fields + f) * pad
                kx = part * k_lo + k
                slot = (i * parts + part) * fields + f
                o_ref[slot] = (acc_ref[f, kx] + c[:, at : at + nz]) * inv_ref[kx]
                copies.append(
                    pltpu.make_async_copy(o_ref.at[slot], o_hbm.at[f, kx], sems.at[slot])
                )
                copies[-1].start()
    for copy in copies:
        copy.wait()


def call(kernel, out_shape, ins, outs, scratch=(), flops=0, bytes_accessed=0, aliases=None):
    return pl.pallas_call(
        kernel,
        out_shape=out_shape,
        in_specs=ins,
        out_specs=outs,
        scratch_shapes=scratch,
        input_output_aliases=aliases or {},
        compiler_params=pltpu.CompilerParams(vmem_limit_bytes=VMEM_GRANT),
        cost_estimate=pl.CostEstimate(
            flops=flops, bytes_accessed=bytes_accessed, transcendentals=0
        ),
    )


def f32(*shape):
    return jax.ShapeDtypeStruct(shape, jnp.float32)


def on_device(rows, cols, species, symbol_x, symbol_y, symbol_z):
    fields, nx, share_in, zs = species.shape
    ny, nz = share_in * rows, zs * cols
    share_x, share_y = nx // rows, ny // cols
    parts = LANES // (fields * zs)
    k_lo = share_x // parts
    assert parts * fields * zs == LANES and k_lo * parts == share_x
    assert share_in == SUBLANES

    hx = basis_table(nx).reshape(rows, parts, k_lo, nx).transpose(1, 0, 2, 3).reshape(nx, nx)
    high, low = split_table(hx)
    hx2 = jnp.asarray(np.concatenate([high, low], axis=1))
    high, low = split_table(basis_table(ny))
    hy2 = jnp.asarray(np.concatenate([high, low], axis=1).reshape(cols, share_y, 2 * ny))
    hz = basis_table(nz).reshape(cols, zs, nz)
    pad = -(-nz // LANES) * LANES
    wz = np.zeros((cols, parts * fields, zs, parts * fields, pad), np.float32)
    for j in range(parts * fields):
        wz[:, j, :, j, :nz] = hz
    wz = wz.reshape(cols, LANES, parts * fields * pad)
    high, low = split_table(wz)
    wz3 = jnp.asarray(np.concatenate([high, low, high], axis=1))

    moved = jnp.transpose(species, (0, 2, 3, 1))
    send = call(
        x_kernel,
        f32(nx // parts * share_in, LANES),
        [HBM, HBM],
        VMEM,
        scratch=[
            pltpu.VMEM(moved.shape, jnp.float32),
            pltpu.VMEM(hx2.shape, jnp.bfloat16),
            pltpu.SemaphoreType.DMA,
            pltpu.SemaphoreType.DMA,
        ],
        flops=6 * nx * nx * fields * share_in * zs,
        bytes_accessed=8 * species.size,
    )(pltpu.with_memory_space_constraint(moved, pltpu.HBM), pltpu.with_memory_space_constraint(hx2, pltpu.HBM))
    got = lax.all_to_all(
        send.reshape(rows, k_lo * share_in, LANES), "row", split_axis=0, concat_axis=0, tiled=True
    ).reshape(rows, k_lo, share_in, LANES)

    size = k_lo // GROUPS
    groups = [range(g * size, (g + 1) * size) for g in range(GROUPS)]
    arrived = []
    for ks in groups:
        pieces = call(
            functools.partial(y_send_kernel, cols, ks),
            [f32(size, share_y, LANES)] * (cols - 1),
            [VMEM, VMEM],
            [VMEM] * (cols - 1),
            flops=6 * share_y * ny * size * LANES * (cols - 1),
            bytes_accessed=8 * species.size // GROUPS,
        )(got, hy2)
        arrived.append(
            [
                lax.ppermute(piece, "col", [(d, (d + step) % cols) for d in range(cols)])
                for step, piece in enumerate(pieces, 1)
            ]
        )
    kept, inverse = call(
        functools.partial(y_keep_kernel, cols),
        [f32(fields, share_x, share_y, nz), f32(share_x, share_y, nz)],
        [VMEM, VMEM, VMEM, SMEM, VMEM, VMEM],
        [VMEM, VMEM],
        scratch=[pltpu.VMEM((ny, LANES), jnp.float32)],
        flops=6 * share_y * ny * k_lo * LANES * 4,
        bytes_accessed=16 * species.size,
    )(got, hy2, wz3, symbol_x, symbol_y.reshape(1, ny), symbol_z.reshape(1, nz))
    out = None
    slots = size * parts * fields
    for ks, parts_in in zip(groups, arrived):
        args = [*parts_in, kept, inverse, wz3] + ([] if out is None else [out])
        out = call(
            functools.partial(z_kernel, cols, k_lo, ks),
            f32(fields, share_x, share_y, nz),
            [VMEM] * (cols + 2) + ([] if out is None else [HBM]),
            HBM,
            scratch=[
                pltpu.VMEM((slots, share_y, nz), jnp.float32),
                pltpu.SemaphoreType.DMA((slots,)),
            ],
            flops=6 * share_y * share_x * fields * nz * nz // GROUPS,
            bytes_accessed=16 * species.size // GROUPS,
            aliases={} if out is None else {cols + 2: 0},
        )(*args)
    return out


def solution(mesh):
    rows, cols = mesh.shape["row"], mesh.shape["col"]
    in_specs = (P(None, None, "row", "col"), P(), P(), P())
    out_specs = P(None, "row", "col", None)
    return jax.shard_map(
        functools.partial(on_device, rows, cols),
        mesh=mesh,
        in_specs=in_specs,
        out_specs=out_specs,
        check_vma=False,
    )
```

```python
import functools

import jax
import jax.numpy as jnp
import numpy as np
from jax import lax
from jax.experimental import pallas as pl
from jax.experimental.pallas import tpu as pltpu
from jax.sharding import PartitionSpec as P

LANES = 128
SUBLANES = 8
VMEM_GRANT = 12 * 2**20
Y_STEP = 2

VMEM = pl.BlockSpec(memory_space=pltpu.VMEM)
SMEM = pl.BlockSpec(memory_space=pltpu.SMEM)
HBM = pl.BlockSpec(memory_space=pltpu.HBM)


def basis_table(count):
    rank = np.arange(count)
    odd = 2 * rank + 1
    angle = np.pi / (4 * count) * (odd[:, None] * odd[None, :] % (8 * count))
    return (np.cos(angle) * (2.0 / count) ** 0.5).astype(np.float32)


def split_table(table):
    high = table.astype(jnp.bfloat16)
    low = (table - high.astype(np.float32)).astype(jnp.bfloat16)
    return high, low


def split(values):
    high = values.astype(jnp.bfloat16)
    low = (values - high.astype(jnp.float32)).astype(jnp.bfloat16)
    return high, low


def dot(left, right):
    return jnp.dot(left, right, preferred_element_type=jnp.float32)


def dot_nt(left, right):
    return lax.dot_general(
        left, right, (((1,), (1,)), ((), ())), preferred_element_type=jnp.float32
    )


def x_kernel(a_hbm, h_hbm, *refs):
    o_refs, (a_ref, h_ref, a_sem, h_sem) = refs[:-4], refs[-4:]
    fields, ys, zs, nx = a_ref.shape
    half = fields * zs
    parts = LANES // half
    rows = h_ref.shape[0] // parts
    own = lax.axis_index("row") if h_hbm.shape[0] > 1 else 0
    copies = [
        pltpu.make_async_copy(h_hbm.at[own], h_ref, h_sem),
        pltpu.make_async_copy(a_hbm, a_ref, a_sem),
    ]
    for copy in copies:
        copy.start()
    for copy in copies:
        copy.wait()
    table = jnp.concatenate([h_ref[...], h_ref[:, :nx]], axis=1)
    share = rows // len(o_refs)
    lane = lax.broadcasted_iota(jnp.int32, (rows, LANES), 1)
    for i in range(0, ys, Y_STEP):
        a = [a_ref[f, y] for y in range(i, i + Y_STEP) for _ in range(parts) for f in range(fields)]
        high, low = split(jnp.concatenate(a, axis=0))
        c = dot_nt(table, jnp.concatenate([high, high, low], axis=1))
        for j in range(Y_STEP):
            mine = c[:, j * LANES : (j + 1) * LANES]
            out = mine[:rows]
            for part in range(1, parts):
                out = jnp.where(lane < part * half, out, mine[part * rows : (part + 1) * rows])
            for n, o_ref in enumerate(o_refs):
                o_ref[pl.ds(i + j, share, stride=ys), :] = out[n * share : (n + 1) * share]


def assemble_kernel(plan, *refs):
    o_refs = refs[len(refs) - len(plan) :]
    for o_ref, blocks in zip(o_refs, plan):
        for at, (source, block) in enumerate(blocks):
            o_ref[at] = refs[source][block]


def assemble(plan, *arrays):
    block = arrays[0].shape[1:]
    return call(
        functools.partial(assemble_kernel, plan),
        [f32(len(blocks), *block) for blocks in plan],
        [VMEM] * len(arrays),
        [VMEM] * len(plan),
        bytes_accessed=8 * sum(map(len, plan)) * block[0] * block[1],
    )(*arrays)


def swap(array, rows, mask):
    return lax.ppermute(array, "row", [(d, d ^ mask) for d in range(rows)])


def exchange_rows(near, far, rows):
    deep = rows // 4
    half = deep // 2
    other = swap(far, rows, 1)
    outer = [[(src, deep + z) for src in (0, 1) for z in zs] for zs in (range(half, deep), range(half))]
    send_far, send_near = assemble(outer, near, other)
    got_far, got_near = swap(send_far, rows, 2), swap(send_near, rows, 2)

    def gathered(zs, first):
        return [[(0, z), (1, z), (2, z - first), (2, half + z - first)] for z in zs]

    pieces = assemble(gathered(range(half, deep), half), near, other, got_far)
    arrived = [swap(piece, rows, 4 * z) for z, piece in enumerate(pieces, half)]
    pieces = assemble(gathered(range(half), 0), near, other, got_near)
    return [pieces[0]] + [swap(piece, rows, 4 * z) for z, piece in enumerate(pieces[1:], 1)] + arrived


def y_products(r_refs, h_ref, target, ks):
    own = lax.axis_index("row") if h_ref.shape[0] > 1 else 0
    table = h_ref[own, target]
    ny = table.shape[1] // 2
    table = jnp.concatenate([table, table[:, :ny]], axis=1)
    outs = []
    for k in ks:
        r = [r_ref[i, k] for r_ref in r_refs for i in range(r_ref.shape[0])]
        high, low = split(jnp.concatenate(r, axis=0))
        outs.append(dot(table, jnp.concatenate([high, high, low], axis=0)))
    return outs


def y_send_kernel(cols, count, *refs):
    r_refs, h_ref, o_refs = refs[:count], refs[count], refs[count + 1 :]
    me = lax.axis_index("col")
    for step, o_ref in enumerate(o_refs, 1):
        target = lax.rem(me + step, cols)
        for k, out in enumerate(y_products(r_refs, h_ref, target, range(o_ref.shape[0]))):
            o_ref[k] = out


def z_products(p, weights):
    high, low = split(p)
    return dot(jnp.concatenate([high, high, low], axis=1), weights)


def y_keep_kernel(count, *refs):
    r_refs = refs[:count]
    h_ref, w_ref, sx_ref, sy_ref, sz_ref, o_ref, inv_ref, sy_scr = refs[count:]
    me = lax.axis_index("col")
    row = lax.axis_index("row")
    fields, share_x, share_y, nz = o_ref.shape
    k_lo = r_refs[0].shape[1]
    parts = share_x // k_lo
    ny = sy_ref.shape[1]
    for i in range(ny // LANES):
        sy_scr[i * LANES : (i + 1) * LANES, :] = jnp.broadcast_to(
            sy_ref[:, i * LANES : (i + 1) * LANES], (LANES, LANES)
        ).T
    sy = sy_scr[pl.ds(me * share_y, share_y), :][:, :1]
    plane = sy + sz_ref[...]
    for k in range(share_x):
        inv_ref[k] = 1.0 / (sx_ref[row * share_x + k] + plane)
    weights = w_ref[me]
    for k, out in enumerate(y_products(r_refs, h_ref, me, range(k_lo))):
        c = z_products(out, weights)
        pad = c.shape[1] // (parts * fields)
        for part in range(parts):
            for f in range(fields):
                at = (part * fields + f) * pad
                o_ref[f, part * k_lo + k] = c[:, at : at + nz]


def z_kernel(cols, *refs):
    p_refs = refs[: cols - 1]
    acc_ref, inv_ref, w_ref = refs[cols - 1 : cols + 2]
    o_hbm, o_ref, sems = refs[-3:]
    me = lax.axis_index("col")
    fields, share_x, share_y, nz = acc_ref.shape
    k_lo = p_refs[0].shape[0]
    parts = share_x // k_lo
    copies = []
    for k in range(k_lo):
        c = None
        for step, p_ref in enumerate(p_refs, 1):
            source = lax.rem(me + cols - step, cols)
            term = z_products(p_ref[k], w_ref[source])
            c = term if c is None else c + term
        pad = c.shape[1] // (parts * fields)
        for part in range(parts):
            for f in range(fields):
                at = (part * fields + f) * pad
                kx = part * k_lo + k
                slot = (k * parts + part) * fields + f
                o_ref[slot] = (acc_ref[f, kx] + c[:, at : at + nz]) * inv_ref[kx]
                copies.append(
                    pltpu.make_async_copy(o_ref.at[slot], o_hbm.at[f, kx], sems.at[slot])
                )
                copies[-1].start()
    for copy in copies:
        copy.wait()


def call(kernel, out_shape, ins, outs, scratch=(), flops=0, bytes_accessed=0):
    return pl.pallas_call(
        kernel,
        out_shape=out_shape,
        in_specs=ins,
        out_specs=outs,
        scratch_shapes=scratch,
        compiler_params=pltpu.CompilerParams(vmem_limit_bytes=VMEM_GRANT),
        cost_estimate=pl.CostEstimate(
            flops=flops, bytes_accessed=bytes_accessed, transcendentals=0
        ),
    )


def f32(*shape):
    return jax.ShapeDtypeStruct(shape, jnp.float32)


def on_device(rows, cols, species, symbol_x, symbol_y, symbol_z):
    fields, nx, share_in, zs = species.shape
    ny, nz = share_in * rows, zs * cols
    share_x, share_y = nx // rows, ny // cols
    parts = LANES // (fields * zs)
    k_lo = share_x // parts
    assert parts * fields * zs == LANES and k_lo * parts == share_x
    assert share_in == SUBLANES

    swaps = rows in (4, 8, 16)
    if swaps:
        deep = rows // 4
        masks = [c + 2 * x + 4 * z for c in (0, 1) for x in (0, 1) for z in range(deep)]
        targets = np.arange(rows)[:, None] ^ np.asarray(masks)
        sources = np.arange(rows)[:, None] ^ np.arange(rows)
    else:
        targets = sources = np.arange(rows)[None]
    devices = targets.shape[0]

    hx = basis_table(nx).reshape(rows, parts, k_lo, nx)[targets]
    high, low = split_table(hx.transpose(0, 2, 1, 3, 4).reshape(devices, nx, nx))
    hx2 = jnp.asarray(np.concatenate([high, low], axis=2))
    hy = basis_table(ny).reshape(cols, share_y, rows, share_in)[:, :, sources]
    high, low = split_table(hy.transpose(2, 0, 1, 3, 4).reshape(devices, cols, share_y, ny))
    hy2 = jnp.asarray(np.concatenate([high, low], axis=3))
    hz = basis_table(nz).reshape(cols, zs, nz)
    pad = -(-nz // LANES) * LANES
    wz = np.zeros((cols, parts * fields, zs, parts * fields, pad), np.float32)
    for j in range(parts * fields):
        wz[:, j, :, j, :nz] = hz
    wz = wz.reshape(cols, LANES, parts * fields * pad)
    high, low = split_table(wz)
    wz3 = jnp.asarray(np.concatenate([high, low, high], axis=1))

    moved = jnp.transpose(species, (0, 2, 3, 1))
    sends = 2 if swaps else 1
    send = call(
        x_kernel,
        [f32(rows * k_lo * share_in // sends, LANES)] * sends,
        [HBM, HBM],
        [VMEM] * sends,
        scratch=[
            pltpu.VMEM(moved.shape, jnp.float32),
            pltpu.VMEM(hx2.shape[1:], jnp.bfloat16),
            pltpu.SemaphoreType.DMA,
            pltpu.SemaphoreType.DMA,
        ],
        flops=6 * nx * nx * fields * share_in * zs,
        bytes_accessed=8 * species.size,
    )(
        pltpu.with_memory_space_constraint(moved, pltpu.HBM),
        pltpu.with_memory_space_constraint(hx2, pltpu.HBM),
    )
    send = [blocks.reshape(rows // sends, k_lo * share_in, LANES) for blocks in send]
    if swaps:
        got = exchange_rows(*send, rows)
    else:
        got = [lax.all_to_all(send[0], "row", split_axis=0, concat_axis=0, tiled=True)]
    got = [blocks.reshape(-1, k_lo, share_in, LANES) for blocks in got]

    pieces = call(
        functools.partial(y_send_kernel, cols, len(got)),
        [f32(k_lo, share_y, LANES)] * (cols - 1),
        [VMEM] * (len(got) + 1),
        [VMEM] * (cols - 1),
        flops=6 * share_y * ny * k_lo * LANES * (cols - 1),
        bytes_accessed=8 * species.size,
    )(*got, hy2)
    arrived = [
        lax.ppermute(piece, "col", [(d, (d + step) % cols) for d in range(cols)])
        for step, piece in enumerate(pieces, 1)
    ]
    kept, inverse = call(
        functools.partial(y_keep_kernel, len(got)),
        [f32(fields, share_x, share_y, nz), f32(share_x, share_y, nz)],
        [VMEM] * (len(got) + 2) + [SMEM, VMEM, VMEM],
        [VMEM, VMEM],
        scratch=[pltpu.VMEM((ny, LANES), jnp.float32)],
        flops=6 * share_y * ny * k_lo * LANES * 4,
        bytes_accessed=16 * species.size,
    )(*got, hy2, wz3, symbol_x, symbol_y.reshape(1, ny), symbol_z.reshape(1, nz))
    slots = share_x * fields
    return call(
        functools.partial(z_kernel, cols),
        f32(fields, share_x, share_y, nz),
        [VMEM] * (cols + 2),
        HBM,
        scratch=[
            pltpu.VMEM((slots, share_y, nz), jnp.float32),
            pltpu.SemaphoreType.DMA((slots,)),
        ],
        flops=6 * share_y * share_x * fields * nz * nz,
        bytes_accessed=16 * species.size,
    )(*arrived, kept, inverse, wz3)


def solution(mesh):
    rows, cols = mesh.shape["row"], mesh.shape["col"]
    in_specs = (P(None, None, "row", "col"), P(), P(), P())
    out_specs = P(None, "row", "col", None)
    return jax.shard_map(
        functools.partial(on_device, rows, cols),
        mesh=mesh,
        in_specs=in_specs,
        out_specs=out_specs,
        check_vma=False,
    )
```

```python
import functools

import jax
import jax.numpy as jnp
import numpy as np
from jax import lax
from jax.experimental import pallas as pl
from jax.experimental.pallas import tpu as pltpu
from jax.sharding import PartitionSpec as P

LANES = 128
SUBLANES = 8
VMEM_GRANT = 12 * 2**20
Y_STEP = 2

VMEM = pl.BlockSpec(memory_space=pltpu.VMEM)
SMEM = pl.BlockSpec(memory_space=pltpu.SMEM)
HBM = pl.BlockSpec(memory_space=pltpu.HBM)


def basis_table(count):
    rank = np.arange(count)
    odd = 2 * rank + 1
    angle = np.pi / (4 * count) * (odd[:, None] * odd[None, :] % (8 * count))
    return (np.cos(angle) * (2.0 / count) ** 0.5).astype(np.float32)


def split_table(table):
    high = table.astype(jnp.bfloat16)
    low = (table - high.astype(np.float32)).astype(jnp.bfloat16)
    return high, low


def split(values):
    high = values.astype(jnp.bfloat16)
    low = (values - high.astype(jnp.float32)).astype(jnp.bfloat16)
    return high, low


def dot(left, right):
    return jnp.dot(left, right, preferred_element_type=jnp.float32)


def dot_nt(left, right):
    return lax.dot_general(
        left, right, (((1,), (1,)), ((), ())), preferred_element_type=jnp.float32
    )


def x_kernel(a_hbm, h_hbm, *refs):
    o_refs, (a_ref, h_ref, a_sem, h_sem) = refs[:-4], refs[-4:]
    fields, ys, zs, nx = a_ref.shape
    half = fields * zs
    parts = LANES // half
    rows = h_ref.shape[0] // parts
    own = lax.axis_index("row") if h_hbm.shape[0] > 1 else 0
    copies = [
        pltpu.make_async_copy(h_hbm.at[own], h_ref, h_sem),
        pltpu.make_async_copy(a_hbm, a_ref, a_sem),
    ]
    for copy in copies:
        copy.start()
    for copy in copies:
        copy.wait()
    table = jnp.concatenate([h_ref[...], h_ref[:, :nx]], axis=1)
    share = rows // len(o_refs)
    lane = lax.broadcasted_iota(jnp.int32, (rows, LANES), 1)
    for i in range(0, ys, Y_STEP):
        a = [a_ref[f, y] for y in range(i, i + Y_STEP) for _ in range(parts) for f in range(fields)]
        high, low = split(jnp.concatenate(a, axis=0))
        c = dot_nt(table, jnp.concatenate([high, high, low], axis=1))
        for j in range(Y_STEP):
            mine = c[:, j * LANES : (j + 1) * LANES]
            out = mine[:rows]
            for part in range(1, parts):
                out = jnp.where(lane < part * half, out, mine[part * rows : (part + 1) * rows])
            for n, o_ref in enumerate(o_refs):
                o_ref[pl.ds(i + j, share, stride=ys), :] = out[n * share : (n + 1) * share]


def assemble_kernel(plan, *refs):
    o_refs = refs[len(refs) - len(plan) :]
    for o_ref, blocks in zip(o_refs, plan):
        for at, (source, block) in enumerate(blocks):
            o_ref[at] = refs[source][block]


def assemble(plan, *arrays):
    block = arrays[0].shape[1:]
    return call(
        functools.partial(assemble_kernel, plan),
        [f32(len(blocks), *block) for blocks in plan],
        [VMEM] * len(arrays),
        [VMEM] * len(plan),
        bytes_accessed=8 * sum(map(len, plan)) * block[0] * block[1],
    )(*arrays)


def swap(array, rows, mask):
    return lax.ppermute(array, "row", [(d, d ^ mask) for d in range(rows)])


def swapped(rows):
    return rows in (4, 8, 16)


def exchange_rows(near, far, rows):
    deep = rows // 4
    half = deep // 2
    other = swap(far, rows, 1)
    outer = [[(src, deep + z) for src in (0, 1) for z in zs] for zs in (range(half, deep), range(half))]
    send_far, send_near = assemble(outer, near, other)
    got_far = swap(send_far, rows, 2)
    got_near = swap(send_near, rows, 2)

    def gathered(zs, first):
        return [[(0, z), (1, z), (2, z - first), (2, half + z - first)] for z in zs]

    pieces = assemble(gathered(range(half, deep), half), near, other, got_far)
    arrived = [swap(piece, rows, 4 * z) for z, piece in enumerate(pieces, half)]
    pieces = assemble(gathered(range(half), 0), near, other, got_near)
    near_by = [swap(piece, rows, 4 * z) for z, piece in enumerate(pieces[1:], 1)]
    return [pieces[0]] + near_by + arrived


def y_products(r_refs, h_ref, target, ks):
    own = lax.axis_index("row") if h_ref.shape[0] > 1 else 0
    table = h_ref[own, target]
    ny = table.shape[1] // 2
    table = jnp.concatenate([table, table[:, :ny]], axis=1)
    outs = []
    for k in ks:
        r = [r_ref[i, k] for r_ref in r_refs for i in range(r_ref.shape[0])]
        high, low = split(jnp.concatenate(r, axis=0))
        outs.append(dot(table, jnp.concatenate([high, high, low], axis=0)))
    return outs


def y_send_kernel(cols, count, *refs):
    r_refs, h_ref, o_refs = refs[:count], refs[count], refs[count + 1 :]
    me = lax.axis_index("col")
    for step, o_ref in enumerate(o_refs, 1):
        target = lax.rem(me + step, cols)
        for k, out in enumerate(y_products(r_refs, h_ref, target, range(o_ref.shape[0]))):
            o_ref[k] = out


def z_products(p, weights):
    high, low = split(p)
    return dot(jnp.concatenate([high, high, low], axis=1), weights)


def y_keep_kernel(count, *refs):
    r_refs = refs[:count]
    h_ref, w_ref, sx_ref, sy_ref, sz_ref, o_ref, inv_ref, sy_scr = refs[count:]
    me = lax.axis_index("col")
    row = lax.axis_index("row")
    fields, share_x, share_y, nz = o_ref.shape
    k_lo = r_refs[0].shape[1]
    parts = share_x // k_lo
    ny = sy_ref.shape[1]
    for i in range(ny // LANES):
        sy_scr[i * LANES : (i + 1) * LANES, :] = jnp.broadcast_to(
            sy_ref[:, i * LANES : (i + 1) * LANES], (LANES, LANES)
        ).T
    sy = sy_scr[pl.ds(me * share_y, share_y), :][:, :1]
    plane = sy + sz_ref[...]
    for k in range(share_x):
        inv_ref[k] = 1.0 / (sx_ref[row * share_x + k] + plane)
    weights = w_ref[me]
    for k, out in enumerate(y_products(r_refs, h_ref, me, range(k_lo))):
        c = z_products(out, weights)
        pad = c.shape[1] // (parts * fields)
        for part in range(parts):
            for f in range(fields):
                at = (part * fields + f) * pad
                o_ref[f, part * k_lo + k] = c[:, at : at + nz]


def z_kernel(cols, *refs):
    p_refs = refs[: cols - 1]
    acc_ref, inv_ref, w_ref = refs[cols - 1 : cols + 2]
    o_hbm, o_ref, sems = refs[-3:]
    me = lax.axis_index("col")
    fields, share_x, _, nz = acc_ref.shape
    k_lo = p_refs[0].shape[0]
    parts = share_x // k_lo
    copies = []
    for k in range(k_lo):
        c = None
        for step, p_ref in enumerate(p_refs, 1):
            source = lax.rem(me + cols - step, cols)
            term = z_products(p_ref[k], w_ref[source])
            c = term if c is None else c + term
        pad = c.shape[1] // (parts * fields)
        for part in range(parts):
            for f in range(fields):
                at = (part * fields + f) * pad
                kx = part * k_lo + k
                slot = (k * parts + part) * fields + f
                o_ref[slot] = (acc_ref[f, kx] + c[:, at : at + nz]) * inv_ref[kx]
                copies.append(
                    pltpu.make_async_copy(o_ref.at[slot], o_hbm.at[f, kx], sems.at[slot])
                )
                copies[-1].start()
    for copy in copies:
        copy.wait()


def call(kernel, out_shape, ins, outs, scratch=(), flops=0, bytes_accessed=0):
    return pl.pallas_call(
        kernel,
        out_shape=out_shape,
        in_specs=ins,
        out_specs=outs,
        scratch_shapes=scratch,
        compiler_params=pltpu.CompilerParams(vmem_limit_bytes=VMEM_GRANT),
        cost_estimate=pl.CostEstimate(
            flops=flops, bytes_accessed=bytes_accessed, transcendentals=0
        ),
    )


def f32(*shape):
    return jax.ShapeDtypeStruct(shape, jnp.float32)


def on_device(rows, cols, species, symbol_x, symbol_y, symbol_z):
    fields, nx, share_in, zs = species.shape
    ny, nz = share_in * rows, zs * cols
    share_x, share_y = nx // rows, ny // cols
    parts = LANES // (fields * zs)
    k_lo = share_x // parts
    assert parts * fields * zs == LANES and k_lo * parts == share_x
    assert share_in == SUBLANES

    swaps = swapped(rows)
    if swaps:
        deep = rows // 4
        masks = [c + 2 * x + 4 * z for c in (0, 1) for x in (0, 1) for z in range(deep)]
        targets = np.arange(rows)[:, None] ^ np.asarray(masks)
        sources = np.arange(rows)[:, None] ^ np.arange(rows)
    else:
        targets = sources = np.arange(rows)[None]
    devices = targets.shape[0]

    hx = basis_table(nx).reshape(rows, parts, k_lo, nx)[targets]
    high, low = split_table(hx.transpose(0, 2, 1, 3, 4).reshape(devices, nx, nx))
    hx2 = jnp.asarray(np.concatenate([high, low], axis=2))
    hy = basis_table(ny).reshape(cols, share_y, rows, share_in)[:, :, sources]
    high, low = split_table(hy.transpose(2, 0, 1, 3, 4).reshape(devices, cols, share_y, ny))
    hy2 = jnp.asarray(np.concatenate([high, low], axis=3))
    hz = basis_table(nz).reshape(cols, zs, nz)
    pad = -(-nz // LANES) * LANES
    wz = np.zeros((cols, parts * fields, zs, parts * fields, pad), np.float32)
    for j in range(parts * fields):
        wz[:, j, :, j, :nz] = hz
    wz = wz.reshape(cols, LANES, parts * fields * pad)
    high, low = split_table(wz)
    wz3 = jnp.asarray(np.concatenate([high, low, high], axis=1))

    moved = jnp.transpose(species, (0, 2, 3, 1))
    sends = 2 if swaps else 1
    send = call(
        x_kernel,
        [f32(rows * k_lo * share_in // sends, LANES)] * sends,
        [HBM, HBM],
        [VMEM] * sends,
        scratch=[
            pltpu.VMEM(moved.shape, jnp.float32),
            pltpu.VMEM(hx2.shape[1:], jnp.bfloat16),
            pltpu.SemaphoreType.DMA,
            pltpu.SemaphoreType.DMA,
        ],
        flops=6 * nx * nx * fields * share_in * zs,
        bytes_accessed=8 * species.size,
    )(
        pltpu.with_memory_space_constraint(moved, pltpu.HBM),
        pltpu.with_memory_space_constraint(hx2, pltpu.HBM),
    )
    send = [blocks.reshape(rows // sends, k_lo * share_in, LANES) for blocks in send]
    if swaps:
        got = exchange_rows(*send, rows)
    else:
        got = [lax.all_to_all(send[0], "row", split_axis=0, concat_axis=0, tiled=True)]
    got = [blocks.reshape(-1, k_lo, share_in, LANES) for blocks in got]

    pieces = call(
        functools.partial(y_send_kernel, cols, len(got)),
        [f32(k_lo, share_y, LANES)] * (cols - 1),
        [VMEM] * (len(got) + 1),
        [VMEM] * (cols - 1),
        flops=6 * share_y * ny * k_lo * LANES * (cols - 1),
        bytes_accessed=8 * species.size,
    )(*got, hy2)
    arrived = [
        lax.ppermute(piece, "col", [(d, (d + step) % cols) for d in range(cols)])
        for step, piece in enumerate(pieces, 1)
    ]
    kept, inverse = call(
        functools.partial(y_keep_kernel, len(got)),
        [f32(fields, share_x, share_y, nz), f32(share_x, share_y, nz)],
        [VMEM] * (len(got) + 2) + [SMEM, VMEM, VMEM],
        [VMEM, VMEM],
        scratch=[pltpu.VMEM((ny, LANES), jnp.float32)],
        flops=6 * share_y * ny * k_lo * LANES * 4,
        bytes_accessed=16 * species.size,
    )(*got, hy2, wz3, symbol_x, symbol_y.reshape(1, ny), symbol_z.reshape(1, nz))
    slots = share_x * fields
    return call(
        functools.partial(z_kernel, cols),
        f32(fields, share_x, share_y, nz),
        [VMEM] * (cols + 2),
        HBM,
        scratch=[
            pltpu.VMEM((slots, share_y, nz), jnp.float32),
            pltpu.SemaphoreType.DMA((slots,)),
        ],
        flops=6 * share_y * share_x * fields * nz * nz,
        bytes_accessed=16 * species.size,
    )(*arrived, kept, inverse, wz3)


def solution(mesh):
    rows, cols = mesh.shape["row"], mesh.shape["col"]
    in_specs = (P(None, None, "row", "col"), P(), P(), P())
    out_specs = P(None, "row", "col", None)

    def step(*args):
        return on_device(rows, cols, *args)

    return jax.shard_map(step, mesh=mesh, in_specs=in_specs, out_specs=out_specs, check_vma=False)
```
